64 devices in a mesh: dp: 8 (over x, y, core), tp: 8 (over z).
Axes of the slice: x: 2, y: 2, z: 8, core: 2. Of those that a mesh axis runs over, the one named last changes fastest.
The devices are a block of a 4x4x8 slice.
Arguments:
- x: bfloat16 [16384, 3072], P('dp'), parts along dimension 0
- dy: bfloat16 [16384, 3072], P('dp'), parts along dimension 0
- gate: bfloat16 [16384, 8192], P('dp', 'tp'), parts along dimension 0
- up: bfloat16 [16384, 8192], P('dp', 'tp'), parts along dimension 0
- w_gate: bfloat16 [3072, 8192], P(None, 'tp')
- w_up: bfloat16 [3072, 8192], P(None, 'tp')
- w_down: bfloat16 [8192, 3072], P('tp')
Outputs:
- output 1: bfloat16 [16384, 3072], P('dp'), parts along dimension 0
- output 2: bfloat16 [24576, 8192], P('dp', 'tp'), parts along dimension 0
- output 3: bfloat16 [24576, 8192], P('dp', 'tp'), parts along dimension 0
- output 4: bfloat16 [65536, 3072], P(('dp', 'tp')), parts along dimension 0
There are 8 independent parts. The reference program is written for one: setup_inputs(seed, part) draws one part's arguments, and reference() takes and returns one part's arrays. A program takes and returns all parts, laid end to end along the dimension named above; an argument that names none is the same for every part.
All inputs are finite; a program needn't handle non-finite values.
Results may differ from the reference program's by a relative error of at most 0.012.
Values are sent between devices in bfloat16 or wider.
A program may use at most 768 MiB of HBM per device.

```python
import jax
import jax.numpy as jnp

ROWS = 2048
D = 3072
FF = 8192


def act(gate, up):
    return jax.nn.silu(gate) * up


def setup_inputs(seed: int = 0, part: int = 0) -> dict:
    kx, ky, ka, kb, kg, ku, kd = jax.random.split(jax.random.key(seed), 7)
    kx, ky, ka, kb = (jax.random.fold_in(k, part) for k in (kx, ky, ka, kb))
    drawn = {
        "x": jax.random.normal(kx, (ROWS, D), jnp.float32),
        "dy": jax.random.normal(ky, (ROWS, D), jnp.float32),
        "gate": jax.random.normal(ka, (ROWS, FF), jnp.float32),
        "up": jax.random.normal(kb, (ROWS, FF), jnp.float32),
        "w_gate": jax.random.normal(kg, (D, FF), jnp.float32) * D**-0.5,
        "w_up": jax.random.normal(ku, (D, FF), jnp.float32) * D**-0.5,
        "w_down": jax.random.normal(kd, (FF, D), jnp.float32) * FF**-0.5,
    }
    return {k: v.astype(jnp.bfloat16) for k, v in drawn.items()}


def reference(x, dy, gate, up, w_gate, w_up, w_down):
    hidden, back = jax.vjp(act, gate.astype(jnp.float32), up.astype(jnp.float32))
    d_hidden = jnp.dot(dy, w_down.T, preferred_element_type=jnp.float32)
    d_gate, d_up = (g.astype(jnp.bfloat16) for g in back(d_hidden))
    dx = jnp.dot(d_gate, w_gate.T, preferred_element_type=jnp.float32) + jnp.dot(d_up, w_up.T, preferred_element_type=jnp.float32)
    dw_gate = jnp.dot(x.T, d_gate, preferred_element_type=jnp.float32)
    dw_up = jnp.dot(x.T, d_up, preferred_element_type=jnp.float32)
    dw_down = jnp.dot(hidden.astype(jnp.bfloat16).T, dy, preferred_element_type=jnp.float32)
    return tuple(g.astype(jnp.bfloat16) for g in (dx, dw_gate, dw_up, dw_down))
```

```python
import functools
import jax
import jax.numpy as jnp
from jax import lax
from jax.experimental import pallas as pl
from jax.experimental.pallas import tpu as pltpu
from jax.sharding import PartitionSpec as P


MESH = pl.DeviceIdType.MESH
F32, BF16 = jnp.float32, jnp.bfloat16
NT = (((1,), (1,)), ((), ()))
TN = (((0,), (0,)), ((), ()))


def rs_kernel(n, dy, gate, up, wd, wg, wu, dg_o, du_o, hid_o, *rest):
    outs, (wd_v, wg_v, wu_v, dy_v, g_v, u_v, dg_v, du_v, h_v, term, slots,
           w_sem, in_sem, d_sem, send_sem, recv_sem, o_sem) = rest[:4], rest[4:]
    me = lax.axis_index("tp")
    sides = (lax.rem(me + 1, n), lax.rem(me + n - 1, n))
    half = dy_v.shape[0] // 2
    cols = slots.shape[3]
    ff, width = wd_v.shape
    fb = 256
    nb = 512
    wp = cols // nb

    def row0(s, d):
        chunk = lax.rem(me + n - 1 - s, n) if d == 0 else lax.rem(me + 1 + s, n)
        return pl.multiple_of(chunk * (2 * half) + d * half, half)

    def inputs(s):
        copies = []
        for d in range(2):
            src, dst = pl.ds(row0(s, d), half), pl.ds(d * half, half)
            for i, (a, v) in enumerate(((dy, dy_v), (gate, g_v), (up, u_v))):
                copies.append(pltpu.make_async_copy(a.at[src], v.at[dst], in_sem.at[d, i]))
        return copies

    def w_down_copy(i):
        at = pl.ds(i * fb, fb)
        return pltpu.make_async_copy(wd.at[at], wd_v.at[at], w_sem.at[0, i])

    def w_in_copies(i):
        at = pl.ds(i * nb, nb)
        return [pltpu.make_async_copy(a.at[at], v.at[at], w_sem.at[1 + k, i]) for k, (a, v) in enumerate(((wg, wg_v), (wu, wu_v)))]

    def d_copies(s):
        copies = []
        for d in range(2):
            src, dst = pl.ds(d * half, half), pl.ds(row0(s, d), half)
            for i, (v, a) in enumerate(((dg_v, dg_o), (du_v, du_o), (h_v, hid_o))):
                copies.append(pltpu.make_async_copy(v.at[src], a.at[dst], d_sem.at[d, i]))
        return copies

    for c in inputs(0):
        c.start()
    for i in range(ff // fb):
        w_down_copy(i).start()
    for i in range(width // nb):
        for c in w_in_copies(i):
            c.start()

    barrier = pltpu.get_barrier_semaphore()
    for side in sides:
        pl.semaphore_signal(barrier, inc=1, device_id={"tp": side}, device_id_type=MESH)
    pl.semaphore_wait(barrier, 2)

    def gradients(s, first):
        for c in inputs(s):
            c.wait()
        if not first:
            for c in d_copies(s):
                c.wait()

        def block(i, _):
            if first:
                w_down_copy(i).wait()
            at = pl.ds(pl.multiple_of(i * fb, fb), fb)
            dh = lax.dot_general(dy_v[...], wd_v[at, :], NT, preferred_element_type=F32)
            g, u = g_v[:, at].astype(F32), u_v[:, at].astype(F32)
            sig = jax.nn.sigmoid(g)
            silu = g * sig
            h_v[:, at] = (silu * u).astype(BF16)
            du_v[:, at] = (dh * silu).astype(BF16)
            dg_v[:, at] = (dh * u * (sig + silu * (1.0 - sig))).astype(BF16)
            return 0

        lax.fori_loop(0, ff // fb, block, 0)
        for c in d_copies(s):
            c.start()

    def product(h, first):
        def block(i, _):
            if first is not None:
                @pl.when(first)
                def _():
                    for c in w_in_copies(h * wp + i):
                        c.wait()
            at = pl.ds(pl.multiple_of(h * cols + i * nb, nb), nb)
            t = lax.dot_general(dg_v[...], wg_v[at, :], NT, preferred_element_type=F32)
            t += lax.dot_general(du_v[...], wu_v[at, :], NT, preferred_element_type=F32)
            term[h, :, pl.ds(pl.multiple_of(i * nb, nb), nb)] = t
            return 0

        lax.fori_loop(0, wp, block, 0)

    def send(s, d, h):
        k = 2 * h + d
        return pltpu.make_async_remote_copy(
            src_ref=slots.at[lax.rem(s + n - 1, n), k],
            dst_ref=slots.at[s, k],
            send_sem=send_sem.at[s, k],
            recv_sem=recv_sem.at[s, k],
            device_id={"tp": sides[d]},
            device_id_type=MESH,
        )

    def results(h):
        copies = []
        for d in range(2):
            for q in range(2):
                r = half // 2
                copies.append(pltpu.make_async_copy(
                    slots.at[n - 2, 2 * h + d, pl.ds(q * r, r)],
                    outs[2 * d + q].at[:, pl.ds(h * cols, cols)], o_sem.at[h, d, q]))
        return copies

    def stream(s, h):
        for d in range(2):
            k = 2 * h + d
            at = pl.ds(d * half, half)

            @pl.when(s == 0)
            def _():
                slots[n - 1, k] = term[h, at].astype(BF16)

            @pl.when(s > 0)
            def _():
                send(s - 1, d, h).wait_recv()
                slots[s - 1, k] = (term[h, at] + slots[s - 1, k].astype(F32)).astype(BF16)

            @pl.when(s < n - 1)
            def _():
                send(s, d, h).start()

    gradients(0, True)
    for c in inputs(1):
        c.start()
    product(0, me >= 0)

    def step(s, _):
        stream(s, 0)
        product(1, s == 0)

        @pl.when(s < n - 1)
        def _():
            gradients(s + 1, False)

        @pl.when(s < n - 2)
        def _():
            for c in inputs(s + 2):
                c.start()

        stream(s, 1)

        @pl.when(s < n - 1)
        def _():
            product(0, None)

        return 0

    lax.fori_loop(0, n, step, 0)
    for h in range(2):
        for c in results(h):
            c.start()
    for c in d_copies(n - 1):
        c.wait()
    for s in range(n - 1):
        for h in range(2):
            for d in range(2):
                send(s, d, h).wait_send()
    for h in range(2):
        for c in results(h):
            c.wait()


def rs(n, dy, gate, up, wd, wg, wu):
    tokens, width = dy.shape
    ff = gate.shape[1]
    rows = tokens // n
    half, cols = rows // 2, width // 2
    any_ = pl.BlockSpec(memory_space=pl.ANY)
    d = jax.ShapeDtypeStruct((tokens, ff), BF16)
    part = jax.ShapeDtypeStruct((half // 2, width), BF16)
    flops = 2 * tokens * ff * width * 3
    return pl.pallas_call(
        functools.partial(rs_kernel, n),
        name="sum_scatter",
        out_shape=[d, d, d] + [part] * 4,
        in_specs=[any_] * 6,
        out_specs=[any_] * 7,
        scratch_shapes=[
            pltpu.VMEM((ff, width), BF16), pltpu.VMEM((width, ff), BF16), pltpu.VMEM((width, ff), BF16),
            pltpu.VMEM((rows, width), BF16), pltpu.VMEM((rows, ff), BF16), pltpu.VMEM((rows, ff), BF16),
            pltpu.VMEM((rows, ff), BF16), pltpu.VMEM((rows, ff), BF16), pltpu.VMEM((rows, ff), BF16),
            pltpu.VMEM((2, rows, cols), F32),
            pltpu.VMEM((n, 4, half, cols), BF16),
            pltpu.SemaphoreType.DMA((3, 8)), pltpu.SemaphoreType.DMA((2, 3)), pltpu.SemaphoreType.DMA((2, 3)),
            pltpu.SemaphoreType.DMA((n - 1, 4)), pltpu.SemaphoreType.DMA((n - 1, 4)), pltpu.SemaphoreType.DMA((2, 2, 2)),
        ],
        compiler_params=pltpu.CompilerParams(collective_id=0, has_side_effects=True, vmem_limit_bytes=60 * 2**20),
        cost_estimate=pl.CostEstimate(flops=flops, bytes_accessed=60 * 2**20, transcendentals=0),
    )(dy, gate, up, wd, wg, wu)


def place(me, n, k, pair, recv, dx_ref, sem, wait):
    r = recv[0].shape[0]
    for d in range(2):
        chunk = lax.rem(me + n - k, n) if d == 0 else lax.rem(me + k, n)
        at = pl.ds(pl.multiple_of((chunk * 4 + 2 * d + pair) * r, r), r)
        copy = pltpu.make_async_copy(recv[d], dx_ref.at[at], sem.at[d])
        if wait:
            copy.wait()
        else:
            copy.start()


def piece_kernel(n, k, pair, steps, shared, *refs):
    *ins, sem = refs
    n_out = len(shared) + 1 if shared else 1
    outs, ins = ins[-n_out:], ins[:-n_out]
    recv, dx_ref = ins[:2], outs[0]
    me = lax.axis_index("tp")
    i = pl.program_id(0)

    @pl.when(i == 0)
    def _():
        place(me, n, k, pair, recv, dx_ref, sem, False)

    if shared:
        lhs = ins[2]
        for rhs, out in zip(ins[3:3 + len(shared)], outs[1:]):
            out[...] = lax.dot_general(lhs[...], rhs[...], TN, preferred_element_type=F32).astype(BF16)

    @pl.when(i == steps - 1)
    def _():
        place(me, n, k, pair, recv, dx_ref, sem, True)


def piece(n, k, pair, recv, dx, dx_shape, work):
    whole = pl.BlockSpec(recv[0].shape, lambda i: (0, 0))
    hbm = pl.BlockSpec(memory_space=pltpu.HBM)
    operands, in_specs = list(recv), [whole, whole]
    out_shape, out_specs, aliases, carry = [dx_shape], [hbm], {}, ()
    steps, flops, shared = 1, 0, ()
    if work is not None:
        lhs, shared, carry, lhs_spec, rhs_spec, out_spec, steps, shape, flops = work
        operands += [lhs, *shared]
        in_specs += [lhs_spec] + [rhs_spec] * len(shared)
        out_shape += [shape] * len(shared)
        out_specs += [out_spec] * len(shared)
        carry = carry or ()
    if dx is not None:
        aliases[len(operands)] = 0
        operands.append(dx)
        in_specs.append(hbm)
    for i, c in enumerate(carry):
        aliases[len(operands)] = 1 + i
        operands.append(c)
        in_specs.append(pl.BlockSpec(memory_space=pl.ANY))
    out = pl.pallas_call(
        functools.partial(piece_kernel, n, k, pair, steps, shared),
        name="piece",
        grid=(steps,),
        out_shape=out_shape,
        in_specs=in_specs,
        out_specs=out_specs,
        scratch_shapes=[pltpu.SemaphoreType.DMA((2,))],
        input_output_aliases=aliases,
        compiler_params=pltpu.CompilerParams(vmem_limit_bytes=36 * 2**20),
        cost_estimate=pl.CostEstimate(flops=max(flops, 10**8), bytes_accessed=8 * 2**20, transcendentals=0),
    )(*operands)
    return out[0], tuple(out[1:])


def work_in(x, dg, du, carry, j, parts):
    tokens, width = x.shape
    ff = dg.shape[1]
    m, nb = width // parts, 256
    return (x, (dg, du), carry, pl.BlockSpec((tokens, m), lambda i: (0, j)), pl.BlockSpec((tokens, nb), lambda i: (0, i)),
            pl.BlockSpec((m, nb), lambda i: (j, i)), ff // nb, jax.ShapeDtypeStruct((width, ff), BF16), 4 * tokens * m * ff)


def work_out(h, dy, carry, j, parts):
    tokens, width = dy.shape
    ff = h.shape[1]
    nb = 256
    steps = width // parts // nb
    return (h, (dy,), carry, pl.BlockSpec((tokens, ff), lambda i: (0, 0)), pl.BlockSpec((tokens, nb), lambda i: (0, j * steps + i)),
            pl.BlockSpec((ff, nb), lambda i: (0, j * steps + i)), steps, jax.ShapeDtypeStruct((ff, width), BF16), 2 * tokens * ff * width // parts)


def solution(mesh):
    n = mesh.shape["tp"]
    right = [(i, (i + 1) % n) for i in range(n)]
    left = [(i, (i - 1) % n) for i in range(n)]

    def step(x, dy, gate, up, w_gate, w_up, w_down):
        dg, du, h, *bufs = rs(n, dy, gate, up, w_down, w_gate, w_up)
        dx_shape = jax.ShapeDtypeStruct(dy.shape, BF16)
        dx = dw = dw_d = None
        todo = [("out", j) for j in range(4)] + [("in", j) for j in range(8)]

        def hop(pair):
            for d, to in ((0, right), (1, left)):
                bufs[2 * d + pair] = lax.ppermute(bufs[2 * d + pair], "tp", to)

        for k in range(n):
            for pair in range(2):
                recv = (bufs[pair], bufs[2 + pair])
                if k < n - 1:
                    hop(pair)
                if not todo:
                    dx, _ = piece(n, k, pair, recv, dx, dx_shape, None)
                else:
                    kind, j = todo.pop(0)
                    if kind == "in":
                        dx, dw = piece(n, k, pair, recv, dx, dx_shape, work_in(x, dg, du, dw, j, 8))
                    else:
                        dx, dw_d = piece(n, k, pair, recv, dx, dx_shape, work_out(h, dy, dw_d, j, 4))
        return dx, *dw, *dw_d

    tokens, columns, rows = P("dp", None), P(None, "tp"), P("tp", None)
    return jax.shard_map(
        step,
        mesh=mesh,
        in_specs=(tokens, tokens, P("dp", "tp"), P("dp", "tp"), columns, columns, rows),
        out_specs=(tokens, P("dp", "tp"), P("dp", "tp"), P(("dp", "tp"), None)),
        check_vma=False,
    )
```
